32 devices in a mesh: slab: 16 (over z, x, core), grp: 2 (over y).
Axes of the slice: x: 2, y: 2, z: 4, core: 2. Of those that a mesh axis runs over, the one named last changes fastest.
Arguments:
- capture: float32 [2, 262144], P(None, ('slab', 'grp')), may hold values from -6 to 6
- dropped: int32 [16], P('slab'), may hold values from 0 to 8191
Outputs:
- max_held: float32 [128, 128, 128], P('slab', 'grp')
- coherent: float32 [2, 128, 128, 128], P(None, 'slab', 'grp')
The draws below stay inside these ranges and needn't reach their ends.
All inputs are finite; a program needn't handle non-finite values.
Results may differ from the reference program's by a relative error of at most 0.0001.
Values sent between devices are 32-bit elements; how exact they have to be, the bound alone decides.
A program may use at most 128 MiB of HBM per device.

```python
import math
import jax
import jax.numpy as jnp
from jax import lax

NCH = 256
HOP = 64
KW = 128
LW = 128
Q = 128
BLOCKS = 2
SAMPLES = 262144
N_SLAB = 16


def set_ends(values, own_key, smallest, top_value):
    shape = values.shape
    place = [jax.random.randint(jax.random.fold_in(own_key, axis), (), 0, shape[axis]) for axis in range(len(shape))]
    values = values.at[tuple(place)].set(smallest)
    longest = shape.index(max(shape))
    place[longest] = (place[longest] + 1) % shape[longest]
    return values.at[tuple(place)].set(top_value)


def steps_of(rng, extent, pieces, low, high):
    def one(position, parts):
        draws = jax.random.uniform(jax.random.fold_in(jax.random.fold_in(rng, 6), position), (parts,), jnp.float32, low / len(pieces), high / len(pieces))
        return jnp.repeat(jnp.exp(draws), extent[position] // parts).reshape((-1,) + (1,) * (len(extent) - position - 1))

    loudness = one(*pieces[0])
    for cut in pieces[1:]:
        loudness = loudness * one(*cut)
    return loudness


def gaussian(rng, dims, scale, bound, pieces=(), kind=jnp.bfloat16):
    loudness = steps_of(rng, dims, pieces, -0.22, 0.18) if pieces else 1.0
    array = jax.random.normal(rng, dims, jnp.float32) * scale * loudness
    return jnp.minimum(jnp.maximum(array, -bound), bound).astype(kind)


def setup_inputs(seed: int = 0) -> dict:
    streams_of = jax.random.split(jax.random.key(seed), 3)
    return {
        "capture": gaussian(streams_of[0], (2, SAMPLES), 1.0, 6.0, ((1, 32),), jnp.float32),
        "dropped": set_ends(jax.random.randint(streams_of[1], (N_SLAB,), 0, Q * HOP), jax.random.fold_in(streams_of[1], 1), 0, (Q * HOP) - 1).astype(jnp.int32),
    }


def reference(capture, dropped):
    lead_hops = NCH // HOP - 1
    slab_hops = BLOCKS * Q
    total_hops = N_SLAB * slab_hops
    padded = jnp.concatenate([jnp.zeros((2, lead_hops * HOP), capture.dtype), capture], axis=1)
    hop_rows = padded.reshape(2, total_hops + lead_hops, HOP)
    frames = jnp.concatenate([hop_rows[:, lag_index:lag_index + total_hops] for lag_index in range(lead_hops + 1)], axis=2)
    tap_index = jnp.arange(NCH, dtype=jnp.int32).astype(jnp.float32)
    window = 0.5 - 0.5 * jnp.cos(2.0 * math.pi * tap_index / NCH)
    scaling = 1.0 / jnp.sqrt(jnp.sum(window * window))
    signal = lax.complex(frames[0] * window, frames[1] * window)
    spectra = jnp.fft.fft(signal, axis=-1)[:, :KW + LW] * scaling
    stamps = jnp.arange(N_SLAB, dtype=jnp.int32) * (BLOCKS * Q * HOP) + jnp.cumsum(dropped).astype(jnp.int32)
    hop_start = jnp.arange(slab_hops, dtype=jnp.int32) * HOP
    clock_mod = ((stamps[:, None] % NCH + hop_start[None, :]) % NCH).reshape(total_hops)
    channels = jnp.arange(KW + LW, dtype=jnp.int32)
    chan_turns = (clock_mod[:, None] * channels[None, :] % NCH).astype(jnp.float32) * (2.0 * math.pi / NCH)
    shifted = spectra * lax.complex(jnp.cos(chan_turns), -jnp.sin(chan_turns))
    shifted = shifted.reshape(N_SLAB, BLOCKS, Q, KW + LW)
    clock_period = Q * HOP
    freq_bins = jnp.arange(Q, dtype=jnp.int32)
    cycle_turns = (freq_bins[None, :] * (stamps % clock_period)[:, None] % clock_period).astype(jnp.float32) * (2.0 * math.pi / clock_period)
    rotation = lax.complex(jnp.cos(cycle_turns), -jnp.sin(cycle_turns))

    def accumulate(state_pair, slab_item):
        largest, running = state_pair
        slab_spectra, slab_rotation = slab_item
        lower_bank = slab_spectra[:, :, :KW]
        upper_bank = slab_spectra[:, :, KW:]
        products = lower_bank[:, :, :, None] * jnp.conj(upper_bank)[:, :, None, :]
        surfaces = jnp.fft.fft(products, axis=1) / math.sqrt(Q)
        largest = jnp.maximum(largest, lax.optimization_barrier(jnp.max(jnp.abs(surfaces), axis=0)))
        running = running + slab_rotation[:, None, None] * lax.optimization_barrier(jnp.sum(surfaces, axis=0))
        return ((largest, running), None)
    empty_surface = jnp.zeros((Q, KW, LW), jnp.float32)
    (largest, running), unused = lax.scan(accumulate, (empty_surface, lax.complex(empty_surface, empty_surface)), (shifted, rotation))
    norm_scale = 1.0 / math.sqrt(N_SLAB * BLOCKS)
    coherent = jnp.stack([jnp.real(running), jnp.imag(running)]) * norm_scale
    return (largest, coherent)
```

```python
import functools
import math

import jax
import jax.numpy as jnp
import numpy as np
from jax import lax
from jax.experimental import pallas as pl
from jax.experimental.pallas import tpu as pltpu
from jax.sharding import PartitionSpec as P

NCH = 256
HOP = 64
KW = 128
LW = 128
Q = 128
BLOCKS = 2
LANES = 128


def split_np(table):
    hi = table.astype(jnp.bfloat16)
    lo = (table - hi.astype(np.float64)).astype(jnp.bfloat16)
    return jnp.asarray(hi), jnp.asarray(lo)


def split(values):
    hi = values.astype(jnp.bfloat16)
    lo = (values - hi.astype(jnp.float32)).astype(jnp.bfloat16)
    return hi, lo


def dft_tables():
    i = np.arange(NCH)
    w = 0.5 - 0.5 * np.cos(2.0 * np.pi * i / NCH)
    w = w / np.sqrt(np.sum(w * w))
    turns = (i[:, None] * i[None, :] % NCH) * (2.0 * np.pi / NCH)
    cos, sin = w[:, None] * np.cos(turns), w[:, None] * np.sin(turns)
    to_real = np.concatenate([cos, sin], 0)
    to_imag = np.concatenate([-sin, cos], 0)
    return to_real, to_imag


def dot3(a_hi, a_lo, b_hi, b_lo, dims):
    dot = functools.partial(
        lax.dot_general, dimension_numbers=(dims, ((), ())), preferred_element_type=jnp.float32
    )
    return dot(a_hi, b_hi) + dot(a_lo, b_hi) + dot(a_hi, b_lo)


def surfaces(
    blk, prev, ty_hi, ty_lo, tx_hi, tx_lo, phy, phx, phq, held, coh, ext, a_hi, a_lo, *, own_bins, own_w, slabs
):
    n = pl.program_id(0)
    rows = Q // 2
    lane = lax.broadcasted_iota(jnp.int32, (rows, LANES), 1)
    low = lane < HOP

    @pl.when(n == 0)
    def _():
        held[...] = jnp.zeros_like(held)
        coh[...] = jnp.zeros_like(coh)
        ext[:, 0:8, :] = jnp.zeros((2, 8, LANES), jnp.float32)

    @pl.when(n > 0)
    def _():
        ext[:, 0:8, :] = prev[0, :, rows - 8 :, :]

    for b in range(BLOCKS):
        ext[:, 8 + b * rows : 8 + (b + 1) * rows, :] = blk[b]
    frames_hi, frames_lo = [], []
    for b in range(BLOCKS):
        at = 8 + b * rows
        even, odd = [], []
        for c in range(2):
            r0 = ext[c, at : at + rows, :]
            r1 = ext[c, at - 1 : at - 1 + rows, :]
            r2 = ext[c, at - 2 : at - 2 + rows, :]
            even += [
                pltpu.roll(jnp.where(low, r1, r2), HOP, 1),
                pltpu.roll(jnp.where(low, r0, r1), HOP, 1),
            ]
            odd += [r1, r0]
        for part in (even, odd):
            hi, lo = split(jnp.concatenate(part, axis=1))
            frames_hi.append(hi)
            frames_lo.append(lo)
    f_hi = jnp.concatenate(frames_hi, axis=0)
    f_lo = jnp.concatenate(frames_lo, axis=0)
    upper = dot3(f_hi, f_lo, ty_hi[...], ty_lo[...], ((1,), (0,)))
    lower = dot3(tx_hi[...], tx_lo[...], f_hi, f_lo, ((1,), (1,)))

    phy_c = [jnp.concatenate([phy[0, p, 0]] * (rows // 8), axis=0) for p in range(2)]
    phy_s = [jnp.concatenate([phy[0, p, 1]] * (rows // 8), axis=0) for p in range(2)]
    for b in range(BLOCKS):
        right = [[], [], [], []]
        for p in range(2):
            part = upper[(2 * b + p) * rows : (2 * b + p + 1) * rows]
            yr, yi = part[:, :LW], part[:, LW:]
            zr = yr * phy_c[p] - yi * phy_s[p]
            zi = yr * phy_s[p] + yi * phy_c[p]
            right[0].append(zr)
            right[1].append(zi)
        zr = jnp.concatenate(right[0], axis=0)
        zi = jnp.concatenate(right[1], axis=0)
        zr_hi, zr_lo = split(zr)
        zi_hi, zi_lo = split(zi)

        def weights(zr, zi):
            return jnp.concatenate(
                [jnp.concatenate([zr, -zi], 1), jnp.concatenate([zi, zr], 1)], axis=0
            )

        y_hi, y_lo = weights(zr_hi, zi_hi), weights(zr_lo, zi_lo)
        xr = lower[:own_w, b * Q : (b + 1) * Q]
        xi = lower[own_w:, b * Q : (b + 1) * Q]
        ur = xr * phx[0, 0] - xi * phx[0, 1]
        ui = xr * phx[0, 1] + xi * phx[0, 0]
        for q in range(own_bins):
            c = phq[0, 0, q : q + 1, :]
            s = phq[0, 1, q : q + 1, :]
            hi, lo = split(jnp.concatenate([ur * c - ui * s, ur * s + ui * c], axis=1))
            a_hi[q * own_w : (q + 1) * own_w, :] = hi
            a_lo[q * own_w : (q + 1) * own_w, :] = lo
        surf = dot3(a_hi[...], a_lo[...], y_hi, y_lo, ((1,), (0,)))
        sr = surf[:, :LW].reshape(own_bins, own_w, LW)
        si = surf[:, LW:].reshape(own_bins, own_w, LW)
        coh[0] += sr
        coh[1] += si
        held[...] = jnp.maximum(held[...], sr * sr + si * si)

    @pl.when(n == pl.num_programs(0) - 1)
    def _():
        held[...] = jnp.sqrt(held[...])
        coh[...] = coh[...] * (1.0 / math.sqrt(slabs * BLOCKS))


def on_device(capture, dropped):
    slab_count = lax.axis_size("slab")
    group_count = lax.axis_size("grp")
    slab = lax.axis_index("slab")
    grp = lax.axis_index("grp")
    own_bins = Q // slab_count
    own_w = KW // group_count
    rows = Q // 2
    local = capture.reshape(2, capture.shape[1] // LANES, LANES)
    every = lax.all_gather(local, ("slab", "grp"), axis=0, tiled=False)
    every = every.reshape(-1, 2, every.shape[2], LANES)
    every = every.reshape(every.shape[0], 2, -1, rows, LANES).swapaxes(1, 2)
    every = every.reshape(slab_count * BLOCKS, 2, rows, LANES)
    drops = lax.all_gather(dropped, "slab", axis=0, tiled=True)
    period = Q * HOP
    stamps = jnp.arange(slab_count, dtype=jnp.int32) * (BLOCKS * period) + jnp.cumsum(drops).astype(
        jnp.int32
    )

    to_real, to_imag = dft_tables()
    ty = np.concatenate([to_real[:, KW:], to_imag[:, KW:]], 1)
    tx = np.stack(
        [
            np.concatenate(
                [to_real[:, g * own_w : (g + 1) * own_w], to_imag[:, g * own_w : (g + 1) * own_w]], 1
            ).T
            for g in range(group_count)
        ]
    ) / math.sqrt(Q)
    ty_hi, ty_lo = split_np(ty)
    tx_hi, tx_lo = (lax.dynamic_index_in_dim(t, grp, 0, False) for t in split_np(tx))

    def turn(k, period):
        a = (k % period).astype(jnp.float32) * (2.0 * math.pi / period)
        return jnp.cos(a), -jnp.sin(a)

    st = stamps[:, None, None]
    j = np.concatenate([np.arange(0, Q, 2), np.arange(1, Q, 2)]).astype(np.int32)
    bins = slab * own_bins + jnp.arange(own_bins, dtype=jnp.int32)
    c, s = turn(bins[None, :, None] * ((st % period + HOP * j[None, None, :]) % period), period)
    phq = jnp.stack([c, s], 1)
    k = grp * own_w + jnp.arange(own_w, dtype=jnp.int32)
    c, s = turn(k[None, :, None] * ((st + HOP * j[None, None, :]) % NCH), NCH)
    phx = jnp.stack([c, s], 1)
    ch = KW + jnp.arange(LW, dtype=jnp.int32)
    jj = jnp.stack([jnp.arange(8) * 2, jnp.arange(8) * 2 + 1]).astype(jnp.int32)
    c, s = turn(
        ch[None, None, None, :] * ((st[..., None] + HOP * jj[None, :, :, None]) % NCH), NCH
    )
    phy = jnp.stack([c, s], 2)

    whole = lambda shape: pl.BlockSpec(shape, lambda n: (0,) * len(shape))
    slabwise = lambda shape: pl.BlockSpec(shape, lambda n: (n,) + (0,) * (len(shape) - 1))
    held, coherent = pl.pallas_call(
        functools.partial(surfaces, own_bins=own_bins, own_w=own_w, slabs=slab_count),
        grid=(slab_count,),
        out_shape=[
            jax.ShapeDtypeStruct((own_bins, own_w, LW), jnp.float32),
            jax.ShapeDtypeStruct((2, own_bins, own_w, LW), jnp.float32),
        ],
        in_specs=[
            slabwise((BLOCKS, 2, rows, LANES)),
            pl.BlockSpec(
                (1, 2, rows, LANES), lambda n: (jnp.maximum(n * BLOCKS - 1, 0), 0, 0, 0)
            ),
            whole((2 * NCH, 2 * LW)),
            whole((2 * NCH, 2 * LW)),
            whole((2 * own_w, 2 * NCH)),
            whole((2 * own_w, 2 * NCH)),
            slabwise((1, 2, 2, 8, LW)),
            slabwise((1, 2, own_w, Q)),
            slabwise((1, 2, own_bins, Q)),
        ],
        out_specs=[whole((own_bins, own_w, LW)), whole((2, own_bins, own_w, LW))],
        scratch_shapes=[
            pltpu.VMEM((2, 8 + BLOCKS * rows, LANES), jnp.float32),
            pltpu.VMEM((own_bins * own_w, 2 * Q), jnp.bfloat16),
            pltpu.VMEM((own_bins * own_w, 2 * Q), jnp.bfloat16),
        ],
    )(every, every, ty_hi, ty_lo, tx_hi, tx_lo, phy, phx, phq)
    return held, coherent


def solution(mesh):
    in_specs = (P(None, ("slab", "grp")), P("slab"))
    out_specs = (P("slab", "grp", None), P(None, "slab", "grp", None))
    return jax.shard_map(
        on_device, mesh=mesh, in_specs=in_specs, out_specs=out_specs, check_vma=False
    )
```

```python
import functools
import math

import jax
import jax.numpy as jnp
import numpy as np
from jax import lax
from jax.experimental import pallas as pl
from jax.experimental.pallas import tpu as pltpu
from jax.sharding import PartitionSpec as P

NCH = 256
HOP = 64
KW = 128
LW = 128
Q = 128
BLOCKS = 2
LANES = 128


def split_np(table):
    hi = table.astype(jnp.bfloat16)
    lo = (table - hi.astype(np.float64)).astype(jnp.bfloat16)
    return jnp.asarray(hi), jnp.asarray(lo)


def split(values):
    hi = values.astype(jnp.bfloat16)
    lo = (values - hi.astype(jnp.float32)).astype(jnp.bfloat16)
    return hi, lo


def dft_tables():
    i = np.arange(NCH)
    w = 0.5 - 0.5 * np.cos(2.0 * np.pi * i / NCH)
    w = w / np.sqrt(np.sum(w * w))
    turns = (i[:, None] * i[None, :] % NCH) * (2.0 * np.pi / NCH)
    cos, sin = w[:, None] * np.cos(turns), w[:, None] * np.sin(turns)
    to_real = np.concatenate([cos, sin], 0)
    to_imag = np.concatenate([-sin, cos], 0)
    return to_real, to_imag


def dot3(a_hi, a_lo, b_hi, b_lo, dims):
    dot = functools.partial(
        lax.dot_general, dimension_numbers=(dims, ((), ())), preferred_element_type=jnp.float32
    )
    return dot(a_hi, b_hi) + dot(a_lo, b_hi) + dot(a_hi, b_lo)


def cos_turns(turns, period):
    v = (jnp.abs(turns.astype(jnp.float32) * (1.0 / period) - 0.5) - 0.25) * (2.0 * math.pi)
    v2 = v * v
    total = jnp.full_like(v, 1.0 / math.factorial(13))
    for order in (11, 9, 7, 5, 3, 1):
        sign = 1.0 if order % 4 == 1 else -1.0
        total = total * v2 + sign / math.factorial(order)
    return total * v


def rotation(turns, period):
    return cos_turns(turns & (period - 1), period), cos_turns((turns + period // 4) & (period - 1), period)


def surfaces(
    own_blk, own_drop, ty_hi, ty_lo, tx_hi, tx_lo, held, coh,
    buf, drops, ext, a_hi, a_lo, send_sem, fwd_sem, recv_sem, dsend_sem, drecv_sem,
    *, slabs, groups, own_bins, own_w
):
    slab, grp = lax.axis_index("slab"), lax.axis_index("grp")
    partner = slab + 1 - 2 * (slab % 2)
    half = slabs // 2
    rows = Q // 2
    local = own_blk.shape[1]
    period = Q * HOP

    barrier = pltpu.get_barrier_semaphore()

    def greet(i, carry):
        pl.semaphore_signal(
            barrier,
            inc=1,
            device_id=((slab + i // groups) % slabs, (grp + i % groups) % groups),
            device_id_type=pl.DeviceIdType.MESH,
        )
        return carry

    lax.fori_loop(1, slabs * groups, greet, 0)

    def to_direct(i):
        return pltpu.make_async_remote_copy(
            src_ref=own_blk,
            dst_ref=buf.at[slab, grp],
            send_sem=send_sem.at[i],
            recv_sem=recv_sem.at[slab, grp],
            device_id=((slab + 2 * (i // groups)) % slabs, (grp + i % groups) % groups),
            device_id_type=pl.DeviceIdType.MESH,
        )

    def drop_copy(i):
        return pltpu.make_async_remote_copy(
            src_ref=own_drop,
            dst_ref=drops.at[slab],
            send_sem=dsend_sem.at[i],
            recv_sem=drecv_sem.at[slab],
            device_id=((slab + i) % slabs, grp),
            device_id_type=pl.DeviceIdType.MESH,
        )

    def arrival(origin, g):
        return pltpu.make_async_remote_copy(
            src_ref=own_blk,
            dst_ref=buf.at[origin, g],
            send_sem=send_sem.at[0],
            recv_sem=recv_sem.at[origin, g],
            device_id=(partner, grp),
            device_id_type=pl.DeviceIdType.MESH,
        )

    def drop_arrival(origin):
        return pltpu.make_async_remote_copy(
            src_ref=own_drop,
            dst_ref=drops.at[origin],
            send_sem=dsend_sem.at[0],
            recv_sem=drecv_sem.at[origin],
            device_id=(partner, grp),
            device_id_type=pl.DeviceIdType.MESH,
        )

    def onward(e, dg):
        origin, g = (slab - 2 * e + slabs) % slabs, (grp + dg) % groups
        return pltpu.make_async_remote_copy(
            src_ref=buf.at[origin, g],
            dst_ref=buf.at[origin, g],
            send_sem=fwd_sem.at[e, dg],
            recv_sem=recv_sem.at[origin, g],
            device_id=(partner, grp),
            device_id_type=pl.DeviceIdType.MESH,
        )

    def own_onward():
        return pltpu.make_async_remote_copy(
            src_ref=own_blk,
            dst_ref=buf.at[slab, grp],
            send_sem=fwd_sem.at[0, 0],
            recv_sem=recv_sem.at[slab, grp],
            device_id=(partner, grp),
            device_id_type=pl.DeviceIdType.MESH,
        )

    def relay(e, first):
        origin = (slab - 2 * e + slabs) % slabs
        for dg in range(first, groups):
            arrival(origin, (grp + dg) % groups).wait_recv()
            onward(e, dg).start()

    drops[slab] = own_drop[...]
    buf[slab, grp] = own_blk[...]
    held[...] = jnp.zeros_like(held)
    coh[...] = jnp.zeros_like(coh)
    pl.semaphore_wait(barrier, slabs * groups - 1)

    def run(copy_of, first, last, act):
        def body(i, carry):
            act(copy_of(i))
            return carry

        lax.fori_loop(first, last, body, 0)

    run(drop_copy, 1, slabs, lambda copy: copy.start())
    own_onward().start()
    run(to_direct, 1, half * groups, lambda copy: copy.start())
    relay(0, 1)
    run(lambda i: drop_arrival((slab + i) % slabs), 1, slabs, lambda copy: copy.wait_recv())
    relay(1, 0)

    lane = lax.broadcasted_iota(jnp.int32, (rows, LANES), 1)
    low = lane < HOP
    jlane = lax.broadcasted_iota(jnp.int32, (8, Q), 1)
    jlane = 2 * (jlane & (rows - 1)) + (jlane >= rows).astype(jnp.int32)
    bins = slab * own_bins + lax.broadcasted_iota(jnp.int32, (own_bins, Q), 0)
    kchan = grp * own_w + lax.broadcasted_iota(jnp.int32, (own_w, Q), 0)
    lchan = KW + lax.broadcasted_iota(jnp.int32, (8, LW), 1)
    jsub = 2 * lax.broadcasted_iota(jnp.int32, (8, LW), 0)

    def spread(array, count):
        return jnp.concatenate([array[:1]] * count, axis=0)

    def step(t, carry):
        n = (slab - t + slabs) % slabs
        before = (n - 1 + slabs) % slabs

        @pl.when((t % 2 == 0) & (t // 2 + 2 < half))
        def _():
            relay(t // 2 + 2, 0)

        @pl.when(t % 2 == 0)
        def _():
            for g in range(groups):
                arrival(before, g).wait_recv()

        stamp = jnp.zeros((8, LANES), jnp.int32) + n * (BLOCKS * period)
        for other in range(slabs):
            stamp = stamp + drops[other] * jnp.where(other <= n, 1, 0)
        at_j = stamp + HOP * jlane
        phq = rotation(bins * (spread(at_j, own_bins) & (period - 1)), period)
        phx = rotation(kchan * (spread(at_j, own_w) & (NCH - 1)), NCH)
        phy = [rotation(lchan * ((stamp + HOP * (jsub + p)) & (NCH - 1)), NCH) for p in range(2)]

        ext[:, 0:8, :] = buf[before, groups - 1, :, local - 8 :, :] * jnp.where(n > 0, 1.0, 0.0)
        for g in range(groups):
            ext[:, 8 + g * local : 8 + (g + 1) * local, :] = buf[n, g]
        frames_hi, frames_lo = [], []
        for b in range(BLOCKS):
            at = 8 + b * rows
            even, odd = [], []
            for c in range(2):
                r0 = ext[c, at : at + rows, :]
                r1 = ext[c, at - 1 : at - 1 + rows, :]
                r2 = ext[c, at - 2 : at - 2 + rows, :]
                even += [
                    pltpu.roll(jnp.where(low, r1, r2), HOP, 1),
                    pltpu.roll(jnp.where(low, r0, r1), HOP, 1),
                ]
                odd += [r1, r0]
            for part in (even, odd):
                hi, lo = split(jnp.concatenate(part, axis=1))
                frames_hi.append(hi)
                frames_lo.append(lo)
        f_hi = jnp.concatenate(frames_hi, axis=0)
        f_lo = jnp.concatenate(frames_lo, axis=0)
        upper = dot3(f_hi, f_lo, ty_hi[...], ty_lo[...], ((1,), (0,)))
        lower = dot3(tx_hi[...], tx_lo[...], f_hi, f_lo, ((1,), (1,)))

        phy_c = [jnp.concatenate([phy[p][0]] * (rows // 8), axis=0) for p in range(2)]
        phy_s = [jnp.concatenate([phy[p][1]] * (rows // 8), axis=0) for p in range(2)]
        for b in range(BLOCKS):
            zrs, zis = [], []
            for p in range(2):
                part = upper[(2 * b + p) * rows : (2 * b + p + 1) * rows]
                yr, yi = part[:, :LW], part[:, LW:]
                zrs.append(yr * phy_c[p] - yi * phy_s[p])
                zis.append(yr * phy_s[p] + yi * phy_c[p])
            zr_hi, zr_lo = split(jnp.concatenate(zrs, axis=0))
            zi_hi, zi_lo = split(jnp.concatenate(zis, axis=0))

            def weights(zr, zi):
                return jnp.concatenate(
                    [jnp.concatenate([zr, -zi], 1), jnp.concatenate([zi, zr], 1)], axis=0
                )

            y_hi, y_lo = weights(zr_hi, zi_hi), weights(zr_lo, zi_lo)
            xr = lower[:own_w, b * Q : (b + 1) * Q]
            xi = lower[own_w:, b * Q : (b + 1) * Q]
            ur = xr * phx[0] - xi * phx[1]
            ui = xr * phx[1] + xi * phx[0]
            for q in range(own_bins):
                c = phq[0][q : q + 1, :]
                s = phq[1][q : q + 1, :]
                hi, lo = split(jnp.concatenate([ur * c - ui * s, ur * s + ui * c], axis=1))
                a_hi[q * own_w : (q + 1) * own_w, :] = hi
                a_lo[q * own_w : (q + 1) * own_w, :] = lo
            surf = dot3(a_hi[...], a_lo[...], y_hi, y_lo, ((1,), (0,)))
            sr = surf[:, :LW].reshape(own_bins, own_w, LW)
            si = surf[:, LW:].reshape(own_bins, own_w, LW)
            coh[0] += sr
            coh[1] += si
            held[...] = jnp.maximum(held[...], sr * sr + si * si)
        return carry

    lax.fori_loop(0, slabs, step, 0)
    held[...] = jnp.sqrt(held[...])
    coh[...] = coh[...] * (1.0 / math.sqrt(slabs * BLOCKS))

    run(drop_copy, 1, slabs, lambda copy: copy.wait_send())
    run(to_direct, 1, half * groups, lambda copy: copy.wait_send())
    own_onward().wait_send()
    run(lambda i: onward(i // groups, i % groups), 1, half * groups, lambda copy: copy.wait_send())


def on_device(capture, dropped):
    slabs = lax.axis_size("slab")
    groups = lax.axis_size("grp")
    grp = lax.axis_index("grp")
    own_bins = Q // slabs
    own_w = KW // groups
    local = capture.shape[1] // LANES
    to_real, to_imag = dft_tables()
    ty = np.concatenate([to_real[:, KW:], to_imag[:, KW:]], 1)
    tx = np.stack(
        [
            np.concatenate(
                [to_real[:, g * own_w : (g + 1) * own_w], to_imag[:, g * own_w : (g + 1) * own_w]], 1
            ).T
            for g in range(groups)
        ]
    ) / math.sqrt(Q)
    ty_hi, ty_lo = split_np(ty)
    tx_hi, tx_lo = (lax.dynamic_index_in_dim(t, grp, 0, False) for t in split_np(tx))
    dma = pltpu.SemaphoreType.DMA
    held, coherent = pl.pallas_call(
        functools.partial(surfaces, slabs=slabs, groups=groups, own_bins=own_bins, own_w=own_w),
        out_shape=[
            jax.ShapeDtypeStruct((own_bins, own_w, LW), jnp.float32),
            jax.ShapeDtypeStruct((2, own_bins, own_w, LW), jnp.float32),
        ],
        in_specs=[pl.BlockSpec(memory_space=pltpu.VMEM)] * 6,
        out_specs=[pl.BlockSpec(memory_space=pltpu.VMEM)] * 2,
        scratch_shapes=[
            pltpu.VMEM((slabs, groups, 2, local, LANES), jnp.float32),
            pltpu.VMEM((slabs, 8, LANES), jnp.int32),
            pltpu.VMEM((2, 8 + BLOCKS * Q // 2, LANES), jnp.float32),
            pltpu.VMEM((own_bins * own_w, 2 * Q), jnp.bfloat16),
            pltpu.VMEM((own_bins * own_w, 2 * Q), jnp.bfloat16),
            dma((slabs // 2 * groups,)),
            dma((slabs // 2, groups)),
            dma((slabs, groups)),
            dma((slabs,)),
            dma((slabs,)),
        ],
        compiler_params=pltpu.CompilerParams(
            collective_id=0, has_side_effects=True, vmem_limit_bytes=48 * 2**20
        ),
    )(
        capture.reshape(2, local, LANES),
        jnp.broadcast_to(dropped.reshape(1, 1), (8, LANES)),
        ty_hi, ty_lo, tx_hi, tx_lo,
    )
    return held, coherent


def solution(mesh):
    in_specs = (P(None, ("slab", "grp")), P("slab"))
    out_specs = (P("slab", "grp", None), P(None, "slab", "grp", None))
    return jax.shard_map(
        on_device, mesh=mesh, in_specs=in_specs, out_specs=out_specs, check_vma=False
    )
```

```python
import functools
import math

import jax
import jax.numpy as jnp
import numpy as np
from jax import lax
from jax.experimental import pallas as pl
from jax.experimental.pallas import tpu as pltpu
from jax.sharding import PartitionSpec as P

NCH = 256
HOP = 64
KW = 128
LW = 128
Q = 128
BLOCKS = 2
LANES = 128


def split_np(table):
    hi = table.astype(jnp.bfloat16)
    lo = (table - hi.astype(np.float64)).astype(jnp.bfloat16)
    return jnp.asarray(hi), jnp.asarray(lo)


def split(values):
    hi = values.astype(jnp.bfloat16)
    lo = (values - hi.astype(jnp.float32)).astype(jnp.bfloat16)
    return hi, lo


def dft_tables():
    i = np.arange(NCH)
    w = 0.5 - 0.5 * np.cos(2.0 * np.pi * i / NCH)
    w = w / np.sqrt(np.sum(w * w))
    turns = (i[:, None] * i[None, :] % NCH) * (2.0 * np.pi / NCH)
    cos, sin = w[:, None] * np.cos(turns), w[:, None] * np.sin(turns)
    to_real = np.concatenate([cos, sin], 0)
    to_imag = np.concatenate([-sin, cos], 0)
    return to_real, to_imag


def dot3(a_hi, a_lo, b_hi, b_lo, dims):
    dot = functools.partial(
        lax.dot_general, dimension_numbers=(dims, ((), ())), preferred_element_type=jnp.float32
    )
    return dot(a_hi, b_hi) + dot(a_lo, b_hi) + dot(a_hi, b_lo)


def cos_turns(turns, period):
    v = (jnp.abs(turns.astype(jnp.float32) * (1.0 / period) - 0.5) - 0.25) * (2.0 * math.pi)
    v2 = v * v
    total = jnp.full_like(v, 1.0 / math.factorial(13))
    for order in (11, 9, 7, 5, 3, 1):
        sign = 1.0 if order % 4 == 1 else -1.0
        total = total * v2 + sign / math.factorial(order)
    return total * v


def rotation(turns, period):
    return cos_turns(turns & (period - 1), period), cos_turns((turns + period // 4) & (period - 1), period)


def flip(index, by, bits):
    total = 0
    for bit in range(bits):
        w = 2**bit
        total = total + ((index // w + by // w) % 2) * w
    return total


def surfaces(
    own_blk, own_info, ty_hi, ty_lo, tx_hi, tx_lo, held, coh,
    buf, infos, ext, a_hi, a_lo, line_sem, x_sem, y_sem, diag_sem, fwd_sem, recv_sem, isend_sem, irecv_sem,
    *, slabs, groups, own_bins, own_w
):
    slab, grp = lax.axis_index("slab"), lax.axis_index("grp")
    bits = slabs.bit_length() - 1
    line = slabs // 4
    rows = Q // 2
    local = own_blk.shape[1]
    period = Q * HOP
    last = groups - 1
    partner = (flip(slab, 1, bits), grp)
    beside = (flip(slab, 2, bits), grp)
    across = (slab, 1 - grp)

    barrier = pltpu.get_barrier_semaphore()

    def greet(i, carry):
        pl.semaphore_signal(
            barrier,
            inc=1,
            device_id=(flip(slab, i // groups, bits), (grp + i) % groups),
            device_id_type=pl.DeviceIdType.MESH,
        )
        return carry

    lax.fori_loop(1, slabs * groups, greet, 0)

    def remote(src, dst, send, recv, target):
        return pltpu.make_async_remote_copy(
            src_ref=src, dst_ref=dst, send_sem=send, recv_sem=recv,
            device_id=target, device_id_type=pl.DeviceIdType.MESH,
        )

    def moved(k, dg, send, target, own=False):
        origin, g = flip(slab, k, bits), (grp + dg) % groups
        src = own_blk if own else buf.at[origin, g]
        return remote(src, buf.at[origin, g], send, recv_sem.at[origin, g], target)

    def arrived(k, dg):
        moved(k, dg, fwd_sem.at[0, 0, 0], partner).wait_recv()

    def info_copy(i):
        target = (flip(slab, i // groups, bits), (grp + i) % groups)
        return remote(own_info, infos.at[slab], isend_sem.at[i], irecv_sem.at[slab], target)

    def info_arrived(origin):
        remote(own_info, infos.at[origin], isend_sem.at[0], irecv_sem.at[origin], partner).wait_recv()

    def line_copy(kz):
        return moved(0, 0, line_sem.at[kz], (flip(slab, 4 * kz, bits), grp), True)

    def column_copies(kz, own=False):
        return [
            moved(4 * kz, 0, x_sem.at[kz], beside, own),
            moved(4 * kz, 0, y_sem.at[kz], across, own),
            moved(4 * kz, 0, fwd_sem.at[kz, 0, 0], partner, own),
        ]

    def forward(kz, kx, dg):
        return moved(4 * kz + 2 * kx, dg, fwd_sem.at[kz, kx, dg], partner)

    def diagonal_y(kz):
        return moved(4 * kz + 2, 0, diag_sem.at[kz], across)

    def diagonal_x(kz):
        return moved(4 * kz, 1, diag_sem.at[kz], beside)

    def from_line(kz):
        arrived(4 * kz, 0)
        for copy in column_copies(kz):
            copy.start()

    def from_x(kz):
        arrived(4 * kz + 2, 0)

        @pl.when(kz % 2 == 1)
        def _():
            diagonal_y(kz).start()

        forward(kz, 1, 0).start()

    def from_y(kz):
        arrived(4 * kz, 1)

        @pl.when(kz % 2 == 0)
        def _():
            diagonal_x(kz).start()

        forward(kz, 0, 1).start()

    def from_diagonal(kz):
        arrived(4 * kz + 2, 1)
        forward(kz, 1, 1).start()

    def run(first, end, act):
        def body(i, carry):
            act(i)
            return carry

        lax.fori_loop(first, end, body, 0)

    buf[slab, grp] = own_blk[...]
    held[...] = jnp.zeros_like(held)
    coh[...] = jnp.zeros_like(coh)
    pl.semaphore_wait(barrier, slabs * groups - 1)

    @pl.when(grp == last)
    def _():
        infos[slab] = own_info[...]
        run(1, slabs * groups, lambda i: info_copy(i).start())

    for copy in column_copies(0, True):
        copy.start()
    run(1, line, lambda kz: line_copy(kz).start())
    zero = slab * 0
    from_x(zero)
    from_y(zero)
    from_line(zero + 1)
    run(1, slabs, lambda i: info_arrived(flip(slab, i, bits)))

    @pl.when(grp != last)
    def _():
        info_arrived(slab)

    lane = lax.broadcasted_iota(jnp.int32, (rows, LANES), 1)
    low = lane < HOP
    jlane = lax.broadcasted_iota(jnp.int32, (8, Q), 1)
    jlane = 2 * (jlane & (rows - 1)) + (jlane >= rows).astype(jnp.int32)
    bins = slab * own_bins + lax.broadcasted_iota(jnp.int32, (own_bins, Q), 0)
    kchan = grp * own_w + lax.broadcasted_iota(jnp.int32, (own_w, Q), 0)
    lchan = KW + lax.broadcasted_iota(jnp.int32, (8, LW), 1)
    jsub = 2 * lax.broadcasted_iota(jnp.int32, (8, LW), 0)

    def spread(array, count):
        return jnp.concatenate([array[:1]] * count, axis=0)

    def step(t, carry):
        n = flip(slab, t, bits)
        before = (n - 1 + slabs) % slabs
        kz, part = t // 4, t % 4

        @pl.when((part == 0) & (kz + 2 < line))
        def _():
            from_line(kz + 2)

        @pl.when(part == 1)
        def _():
            from_diagonal(kz)

        @pl.when((part == 2) & (kz + 1 < line))
        def _():
            from_x(kz + 1)

        @pl.when((part == 3) & (kz + 1 < line))
        def _():
            from_y(kz + 1)

        @pl.when(part % 2 == 1)
        def _():
            arrived(t, 0)
            arrived(t, 1)

        drops = jnp.zeros((1, LANES), jnp.float32)
        for other in range(slabs):
            drops = drops + infos[other, 4:5, :] * jnp.where(other <= n, 1.0, 0.0)
        stamp = jnp.concatenate([drops.astype(jnp.int32) + n * (BLOCKS * period)] * 8, axis=0)
        at_j = stamp + HOP * jlane
        phq = rotation(bins * (spread(at_j, own_bins) & (period - 1)), period)
        phx = rotation(kchan * (spread(at_j, own_w) & (NCH - 1)), NCH)
        phy = [rotation(lchan * ((stamp + HOP * (jsub + p)) & (NCH - 1)), NCH) for p in range(2)]

        for c in range(2):
            ext[c, 6:8, :] = infos[before, 2 * c : 2 * c + 2, :] * jnp.where(n > 0, 1.0, 0.0)
        for g in range(groups):
            ext[:, 8 + g * local : 8 + (g + 1) * local, :] = buf[n, g]
        frames_hi, frames_lo = [], []
        for b in range(BLOCKS):
            at = 8 + b * rows
            even, odd = [], []
            for c in range(2):
                r0 = ext[c, at : at + rows, :]
                r1 = ext[c, at - 1 : at - 1 + rows, :]
                r2 = ext[c, at - 2 : at - 2 + rows, :]
                even += [
                    pltpu.roll(jnp.where(low, r1, r2), HOP, 1),
                    pltpu.roll(jnp.where(low, r0, r1), HOP, 1),
                ]
                odd += [r1, r0]
            for part in (even, odd):
                hi, lo = split(jnp.concatenate(part, axis=1))
                frames_hi.append(hi)
                frames_lo.append(lo)
        f_hi = jnp.concatenate(frames_hi, axis=0)
        f_lo = jnp.concatenate(frames_lo, axis=0)
        upper = dot3(f_hi, f_lo, ty_hi[...], ty_lo[...], ((1,), (0,)))
        lower = dot3(tx_hi[...], tx_lo[...], f_hi, f_lo, ((1,), (1,)))

        phy_c = [jnp.concatenate([phy[p][0]] * (rows // 8), axis=0) for p in range(2)]
        phy_s = [jnp.concatenate([phy[p][1]] * (rows // 8), axis=0) for p in range(2)]
        for b in range(BLOCKS):
            zrs, zis = [], []
            for p in range(2):
                part = upper[(2 * b + p) * rows : (2 * b + p + 1) * rows]
                yr, yi = part[:, :LW], part[:, LW:]
                zrs.append(yr * phy_c[p] - yi * phy_s[p])
                zis.append(yr * phy_s[p] + yi * phy_c[p])
            zr_hi, zr_lo = split(jnp.concatenate(zrs, axis=0))
            zi_hi, zi_lo = split(jnp.concatenate(zis, axis=0))

            def weights(zr, zi):
                return jnp.concatenate(
                    [jnp.concatenate([zr, -zi], 1), jnp.concatenate([zi, zr], 1)], axis=0
                )

            y_hi, y_lo = weights(zr_hi, zi_hi), weights(zr_lo, zi_lo)
            xr = lower[:own_w, b * Q : (b + 1) * Q]
            xi = lower[own_w:, b * Q : (b + 1) * Q]
            ur = xr * phx[0] - xi * phx[1]
            ui = xr * phx[1] + xi * phx[0]
            for q in range(own_bins):
                c = phq[0][q : q + 1, :]
                s = phq[1][q : q + 1, :]
                hi, lo = split(jnp.concatenate([ur * c - ui * s, ur * s + ui * c], axis=1))
                a_hi[q * own_w : (q + 1) * own_w, :] = hi
                a_lo[q * own_w : (q + 1) * own_w, :] = lo
            surf = dot3(a_hi[...], a_lo[...], y_hi, y_lo, ((1,), (0,)))
            sr = surf[:, :LW].reshape(own_bins, own_w, LW)
            si = surf[:, LW:].reshape(own_bins, own_w, LW)
            coh[0] += sr
            coh[1] += si
            held[...] = jnp.maximum(held[...], sr * sr + si * si)
        return carry

    lax.fori_loop(0, slabs, step, 0)
    held[...] = jnp.sqrt(held[...])
    coh[...] = coh[...] * (1.0 / math.sqrt(slabs * BLOCKS))

    @pl.when(grp == last)
    def _():
        run(1, slabs * groups, lambda i: info_copy(i).wait_send())

    run(1, line, lambda kz: line_copy(kz).wait_send())

    def sent(kz):
        for copy in column_copies(kz):
            copy.wait_send()
        diagonal_x(kz).wait_send()
        for kx, dg in ((0, 1), (1, 0), (1, 1)):
            forward(kz, kx, dg).wait_send()

    run(0, line, sent)


def on_device(capture, dropped):
    slabs = lax.axis_size("slab")
    groups = lax.axis_size("grp")
    grp = lax.axis_index("grp")
    own_bins = Q // slabs
    own_w = KW // groups
    local = capture.shape[1] // LANES
    to_real, to_imag = dft_tables()
    ty = np.concatenate([to_real[:, KW:], to_imag[:, KW:]], 1)
    tx = np.stack(
        [
            np.concatenate(
                [to_real[:, g * own_w : (g + 1) * own_w], to_imag[:, g * own_w : (g + 1) * own_w]], 1
            ).T
            for g in range(groups)
        ]
    ) / math.sqrt(Q)
    ty_hi, ty_lo = split_np(ty)
    tx_hi, tx_lo = (lax.dynamic_index_in_dim(t, grp, 0, False) for t in split_np(tx))
    blocks = capture.reshape(2, local, LANES)
    tail = capture[:, capture.shape[1] - 2 * LANES :].reshape(4, LANES)
    drop = jnp.broadcast_to(dropped.astype(jnp.float32).reshape(1, 1), (4, LANES))
    info = jnp.concatenate([tail, drop], axis=0)
    dma = pltpu.SemaphoreType.DMA
    held, coherent = pl.pallas_call(
        functools.partial(surfaces, slabs=slabs, groups=groups, own_bins=own_bins, own_w=own_w),
        out_shape=[
            jax.ShapeDtypeStruct((own_bins, own_w, LW), jnp.float32),
            jax.ShapeDtypeStruct((2, own_bins, own_w, LW), jnp.float32),
        ],
        in_specs=[pl.BlockSpec(memory_space=pltpu.VMEM)] * 6,
        out_specs=[pl.BlockSpec(memory_space=pltpu.VMEM)] * 2,
        scratch_shapes=[
            pltpu.VMEM((slabs, groups, 2, local, LANES), jnp.float32),
            pltpu.VMEM((slabs, 8, LANES), jnp.float32),
            pltpu.VMEM((2, 8 + BLOCKS * Q // 2, LANES), jnp.float32),
            pltpu.VMEM((own_bins * own_w, 2 * Q), jnp.bfloat16),
            pltpu.VMEM((own_bins * own_w, 2 * Q), jnp.bfloat16),
            dma((slabs // 4,)),
            dma((slabs // 4,)),
            dma((slabs // 4,)),
            dma((slabs // 4,)),
            dma((slabs // 4, 2, groups)),
            dma((slabs, groups)),
            dma((slabs * groups,)),
            dma((slabs,)),
        ],
        compiler_params=pltpu.CompilerParams(
            collective_id=0, has_side_effects=True, vmem_limit_bytes=48 * 2**20
        ),
    )(
        blocks,
        info,
        ty_hi, ty_lo, tx_hi, tx_lo,
    )
    return held, coherent


def solution(mesh):
    in_specs = (P(None, ("slab", "grp")), P("slab"))
    out_specs = (P("slab", "grp", None), P(None, "slab", "grp", None))
    return jax.shard_map(
        on_device, mesh=mesh, in_specs=in_specs, out_specs=out_specs, check_vma=False
    )
```

```python
import functools
import math

import jax
import jax.numpy as jnp
import numpy as np
from jax import lax
from jax.experimental import pallas as pl
from jax.experimental.pallas import tpu as pltpu
from jax.sharding import PartitionSpec as P

NCH = 256
HOP = 64
KW = 128
LW = 128
Q = 128
BLOCKS = 2
LANES = 128


def split_np(table):
    hi = table.astype(jnp.bfloat16)
    lo = (table - hi.astype(np.float64)).astype(jnp.bfloat16)
    return jnp.asarray(hi), jnp.asarray(lo)


def split(values):
    hi = values.astype(jnp.bfloat16)
    lo = (values - hi.astype(jnp.float32)).astype(jnp.bfloat16)
    return hi, lo


def dft_tables():
    i = np.arange(NCH)
    w = 0.5 - 0.5 * np.cos(2.0 * np.pi * i / NCH)
    w = w / np.sqrt(np.sum(w * w))
    turns = (i[:, None] * i[None, :] % NCH) * (2.0 * np.pi / NCH)
    cos, sin = w[:, None] * np.cos(turns), w[:, None] * np.sin(turns)
    to_real = np.concatenate([cos, sin], 0)
    to_imag = np.concatenate([-sin, cos], 0)
    return to_real, to_imag


def dot3(a_hi, a_lo, b_hi, b_lo, dims):
    dot = functools.partial(
        lax.dot_general, dimension_numbers=(dims, ((), ())), preferred_element_type=jnp.float32
    )
    return dot(a_hi, b_hi) + dot(a_lo, b_hi) + dot(a_hi, b_lo)


def cos_turns(turns, period):
    v = (jnp.abs(turns.astype(jnp.float32) * (1.0 / period) - 0.5) - 0.25) * (2.0 * math.pi)
    v2 = v * v
    total = jnp.full_like(v, 1.0 / math.factorial(13))
    for order in (11, 9, 7, 5, 3, 1):
        sign = 1.0 if order % 4 == 1 else -1.0
        total = total * v2 + sign / math.factorial(order)
    return total * v


def rotation(turns, period):
    return cos_turns(turns & (period - 1), period), cos_turns((turns + period // 4) & (period - 1), period)


def flip(index, by, bits):
    total = 0
    for bit in range(bits):
        w = 2**bit
        total = total + ((index // w + by // w) % 2) * w
    return total


def surfaces(
    own_blk, own_info, ty_hi, ty_lo, tx_hi, tx_lo, held, coh,
    buf, infos, ext, *rest,
    slabs, groups, own_bins, own_w
):
    slots = rest[:4], rest[4:8]
    line_sem, x_sem, y_sem, diag_sem, fwd_sem, recv_sem, isend_sem, irecv_sem = rest[8:]
    slab, grp = lax.axis_index("slab"), lax.axis_index("grp")
    bits = slabs.bit_length() - 1
    line = slabs // 4
    rows = Q // 2
    local = own_blk.shape[1]
    period = Q * HOP
    last = groups - 1
    partner = (flip(slab, 1, bits), grp)
    beside = (flip(slab, 2, bits), grp)
    across = (slab, 1 - grp)

    barrier = pltpu.get_barrier_semaphore()

    def greet(i, carry):
        pl.semaphore_signal(
            barrier,
            inc=1,
            device_id=(flip(slab, i // groups, bits), (grp + i) % groups),
            device_id_type=pl.DeviceIdType.MESH,
        )
        return carry

    lax.fori_loop(1, slabs * groups, greet, 0)

    def remote(src, dst, send, recv, target):
        return pltpu.make_async_remote_copy(
            src_ref=src, dst_ref=dst, send_sem=send, recv_sem=recv,
            device_id=target, device_id_type=pl.DeviceIdType.MESH,
        )

    def moved(k, dg, send, target, own=False):
        origin, g = flip(slab, k, bits), (grp + dg) % groups
        src = own_blk if own else buf.at[origin, g]
        return remote(src, buf.at[origin, g], send, recv_sem.at[origin, g], target)

    def arrived(k, dg):
        moved(k, dg, fwd_sem.at[0, 0, 0], partner).wait_recv()

    def info_copy(i):
        target = (flip(slab, i // groups, bits), (grp + i) % groups)
        return remote(own_info, infos.at[slab], isend_sem.at[i], irecv_sem.at[slab], target)

    def info_arrived(origin):
        remote(own_info, infos.at[origin], isend_sem.at[0], irecv_sem.at[origin], partner).wait_recv()

    def line_copy(kz):
        return moved(0, 0, line_sem.at[kz], (flip(slab, 4 * kz, bits), grp), True)

    def column_copies(kz, own=False):
        return [
            moved(4 * kz, 0, x_sem.at[kz], beside, own),
            moved(4 * kz, 0, y_sem.at[kz], across, own),
            moved(4 * kz, 0, fwd_sem.at[kz, 0, 0], partner, own),
        ]

    def forward(kz, kx, dg):
        return moved(4 * kz + 2 * kx, dg, fwd_sem.at[kz, kx, dg], partner)

    def diagonal_y(kz):
        return moved(4 * kz + 2, 0, diag_sem.at[kz], across)

    def diagonal_x(kz):
        return moved(4 * kz, 1, diag_sem.at[kz], beside)

    def from_line(kz):
        arrived(4 * kz, 0)
        for copy in column_copies(kz):
            copy.start()

    def from_x(kz):
        arrived(4 * kz + 2, 0)

        @pl.when(kz % 2 == 1)
        def _():
            diagonal_y(kz).start()

        forward(kz, 1, 0).start()

    def from_y(kz):
        arrived(4 * kz, 1)

        @pl.when(kz % 2 == 0)
        def _():
            diagonal_x(kz).start()

        forward(kz, 0, 1).start()

    def from_diagonal(kz):
        arrived(4 * kz + 2, 1)
        forward(kz, 1, 1).start()

    def run(first, end, act):
        def body(i, carry):
            act(i)
            return carry

        lax.fori_loop(first, end, body, 0)

    buf[slab, grp] = own_blk[...]
    held[...] = jnp.zeros_like(held)
    coh[...] = jnp.zeros_like(coh)
    pl.semaphore_wait(barrier, slabs * groups - 1)

    @pl.when(grp == last)
    def _():
        infos[slab] = own_info[...]
        run(1, slabs * groups, lambda i: info_copy(i).start())

    for copy in column_copies(0, True):
        copy.start()
    run(1, line, lambda kz: line_copy(kz).start())
    zero = slab * 0
    from_x(zero)
    from_y(zero)
    run(1, slabs, lambda i: info_arrived(flip(slab, i, bits)))

    @pl.when(grp != last)
    def _():
        info_arrived(slab)

    lane = lax.broadcasted_iota(jnp.int32, (rows, LANES), 1)
    low = lane < HOP
    jlane = lax.broadcasted_iota(jnp.int32, (8, Q), 1)
    jlane = 2 * (jlane & (rows - 1)) + (jlane >= rows).astype(jnp.int32)
    bins = slab * own_bins + lax.broadcasted_iota(jnp.int32, (own_bins, Q), 0)
    kchan = grp * own_w + lax.broadcasted_iota(jnp.int32, (own_w, Q), 0)
    lchan = KW + lax.broadcasted_iota(jnp.int32, (8, LW), 1)
    jsub = 2 * lax.broadcasted_iota(jnp.int32, (8, LW), 0)

    def spread(array, count):
        return jnp.concatenate([array[:1]] * count, axis=0)

    def events(t):
        @pl.when((t % 2 == 0) & (t // 2 + 1 < line))
        def _():
            from_line(t // 2 + 1)

        @pl.when((t % 2 == 1) & (t >= 3) & (t // 2 < line))
        def _():
            from_y(t // 2)
            from_x(t // 2)

        @pl.when((t % 3 == 2) & (t // 3 < line))
        def _():
            from_diagonal(t // 3)

        @pl.when(t % 2 == 1)
        def _():
            arrived(t, 0)
            arrived(t, 1)

    def prepare(t, slot):
        n = flip(slab, t, bits)
        before = (n - 1 + slabs) % slabs
        a_hi, a_lo, w_hi, w_lo = slot
        drops = jnp.zeros((1, LANES), jnp.float32)
        for other in range(slabs):
            drops = drops + infos[other, 4:5, :] * jnp.where(other <= n, 1.0, 0.0)
        stamp = jnp.concatenate([drops.astype(jnp.int32) + n * (BLOCKS * period)] * 8, axis=0)
        at_j = stamp + HOP * jlane
        phq = rotation(bins * (spread(at_j, own_bins) & (period - 1)), period)
        phx = rotation(kchan * (spread(at_j, own_w) & (NCH - 1)), NCH)
        phy = [rotation(lchan * ((stamp + HOP * (jsub + p)) & (NCH - 1)), NCH) for p in range(2)]

        for c in range(2):
            ext[c, 6:8, :] = infos[before, 2 * c : 2 * c + 2, :] * jnp.where(n > 0, 1.0, 0.0)
        for g in range(groups):
            ext[:, 8 + g * local : 8 + (g + 1) * local, :] = buf[n, g]
        frames_hi, frames_lo = [], []
        for b in range(BLOCKS):
            at = 8 + b * rows
            even, odd = [], []
            for c in range(2):
                r0 = ext[c, at : at + rows, :]
                r1 = ext[c, at - 1 : at - 1 + rows, :]
                r2 = ext[c, at - 2 : at - 2 + rows, :]
                even += [
                    pltpu.roll(jnp.where(low, r1, r2), HOP, 1),
                    pltpu.roll(jnp.where(low, r0, r1), HOP, 1),
                ]
                odd += [r1, r0]
            for part in (even, odd):
                hi, lo = split(jnp.concatenate(part, axis=1))
                frames_hi.append(hi)
                frames_lo.append(lo)
        f_hi = jnp.concatenate(frames_hi, axis=0)
        f_lo = jnp.concatenate(frames_lo, axis=0)
        upper = dot3(f_hi, f_lo, ty_hi[...], ty_lo[...], ((1,), (0,)))
        lower = dot3(tx_hi[...], tx_lo[...], f_hi, f_lo, ((1,), (1,)))

        phy_c = [jnp.concatenate([phy[p][0]] * (rows // 8), axis=0) for p in range(2)]
        phy_s = [jnp.concatenate([phy[p][1]] * (rows // 8), axis=0) for p in range(2)]
        for b in range(BLOCKS):
            zrs, zis = [], []
            for p in range(2):
                part = upper[(2 * b + p) * rows : (2 * b + p + 1) * rows]
                yr, yi = part[:, :LW], part[:, LW:]
                zrs.append(yr * phy_c[p] - yi * phy_s[p])
                zis.append(yr * phy_s[p] + yi * phy_c[p])
            zr_hi, zr_lo = split(jnp.concatenate(zrs, axis=0))
            zi_hi, zi_lo = split(jnp.concatenate(zis, axis=0))

            def weights(zr, zi):
                return jnp.concatenate(
                    [jnp.concatenate([zr, -zi], 1), jnp.concatenate([zi, zr], 1)], axis=0
                )

            w_hi[b] = weights(zr_hi, zi_hi)
            w_lo[b] = weights(zr_lo, zi_lo)
            xr = lower[:own_w, b * Q : (b + 1) * Q]
            xi = lower[own_w:, b * Q : (b + 1) * Q]
            ur = xr * phx[0] - xi * phx[1]
            ui = xr * phx[1] + xi * phx[0]
            for q in range(own_bins):
                c = phq[0][q : q + 1, :]
                s = phq[1][q : q + 1, :]
                hi, lo = split(jnp.concatenate([ur * c - ui * s, ur * s + ui * c], axis=1))
                a_hi[b, q * own_w : (q + 1) * own_w, :] = hi
                a_lo[b, q * own_w : (q + 1) * own_w, :] = lo

    def accumulate(slot):
        a_hi, a_lo, w_hi, w_lo = slot
        surf = [dot3(a_hi[b], a_lo[b], w_hi[b], w_lo[b], ((1,), (0,))) for b in range(BLOCKS)]
        largest, real, imag = held[...], coh[0], coh[1]
        for part in surf:
            sr = part[:, :LW].reshape(own_bins, own_w, LW)
            si = part[:, LW:].reshape(own_bins, own_w, LW)
            real, imag = real + sr, imag + si
            largest = jnp.maximum(largest, sr * sr + si * si)
        held[...] = largest
        coh[0] = real
        coh[1] = imag

    def pair(i, carry):
        t = 2 * i
        events(t + 1)
        prepare(t + 1, slots[1])
        accumulate(slots[0])
        events(t + 2)
        prepare(t + 2, slots[0])
        accumulate(slots[1])
        return carry

    events(zero)
    prepare(zero, slots[0])
    lax.fori_loop(0, slabs // 2 - 1, pair, 0)
    events(zero + slabs - 1)
    prepare(zero + slabs - 1, slots[1])
    accumulate(slots[0])
    accumulate(slots[1])
    held[...] = jnp.sqrt(held[...])
    coh[...] = coh[...] * (1.0 / math.sqrt(slabs * BLOCKS))

    @pl.when(grp == last)
    def _():
        run(1, slabs * groups, lambda i: info_copy(i).wait_send())

    run(1, line, lambda kz: line_copy(kz).wait_send())

    def sent(kz):
        for copy in column_copies(kz):
            copy.wait_send()
        diagonal_x(kz).wait_send()
        for kx, dg in ((0, 1), (1, 0), (1, 1)):
            forward(kz, kx, dg).wait_send()

    run(0, line, sent)


def on_device(capture, dropped):
    slabs = lax.axis_size("slab")
    groups = lax.axis_size("grp")
    grp = lax.axis_index("grp")
    own_bins = Q // slabs
    own_w = KW // groups
    local = capture.shape[1] // LANES
    to_real, to_imag = dft_tables()
    ty = np.concatenate([to_real[:, KW:], to_imag[:, KW:]], 1)
    tx = np.stack(
        [
            np.concatenate(
                [to_real[:, g * own_w : (g + 1) * own_w], to_imag[:, g * own_w : (g + 1) * own_w]], 1
            ).T
            for g in range(groups)
        ]
    ) / math.sqrt(Q)
    ty_hi, ty_lo = split_np(ty)
    tx_hi, tx_lo = (lax.dynamic_index_in_dim(t, grp, 0, False) for t in split_np(tx))
    blocks = capture.reshape(2, local, LANES)
    tail = capture[:, capture.shape[1] - 2 * LANES :].reshape(4, LANES)
    drop = jnp.broadcast_to(dropped.astype(jnp.float32).reshape(1, 1), (4, LANES))
    info = jnp.concatenate([tail, drop], axis=0)
    dma = pltpu.SemaphoreType.DMA
    slot = [pltpu.VMEM((BLOCKS, own_bins * own_w, 2 * Q), jnp.bfloat16)] * 2
    slot = slot + [pltpu.VMEM((BLOCKS, 2 * Q, 2 * LW), jnp.bfloat16)] * 2
    held, coherent = pl.pallas_call(
        functools.partial(surfaces, slabs=slabs, groups=groups, own_bins=own_bins, own_w=own_w),
        out_shape=[
            jax.ShapeDtypeStruct((own_bins, own_w, LW), jnp.float32),
            jax.ShapeDtypeStruct((2, own_bins, own_w, LW), jnp.float32),
        ],
        in_specs=[pl.BlockSpec(memory_space=pltpu.VMEM)] * 6,
        out_specs=[pl.BlockSpec(memory_space=pltpu.VMEM)] * 2,
        scratch_shapes=[
            pltpu.VMEM((slabs, groups, 2, local, LANES), jnp.float32),
            pltpu.VMEM((slabs, 8, LANES), jnp.float32),
            pltpu.VMEM((2, 8 + BLOCKS * Q // 2, LANES), jnp.float32),
            *slot,
            *slot,
            dma((slabs // 4,)),
            dma((slabs // 4,)),
            dma((slabs // 4,)),
            dma((slabs // 4,)),
            dma((slabs // 4, 2, groups)),
            dma((slabs, groups)),
            dma((slabs * groups,)),
            dma((slabs,)),
        ],
        compiler_params=pltpu.CompilerParams(
            collective_id=0, has_side_effects=True, vmem_limit_bytes=48 * 2**20
        ),
    )(
        blocks,
        info,
        ty_hi, ty_lo, tx_hi, tx_lo,
    )
    return held, coherent


def solution(mesh):
    in_specs = (P(None, ("slab", "grp")), P("slab"))
    out_specs = (P("slab", "grp", None), P(None, "slab", "grp", None))
    return jax.shard_map(
        on_device, mesh=mesh, in_specs=in_specs, out_specs=out_specs, check_vma=False
    )
```
